32 devices in a mesh: copies: 2 (over y), grid: 4 (over z), slab: 4 (over x, core).
Axes of the slice: x: 2, y: 2, z: 4, core: 2. Of those that a mesh axis runs over, the one named last changes fastest.
Arguments:
- field: float32 [8, 128, 64, 128], P(('copies', 'grid'), 'slab'), parts along dimension 0, may hold values from -6 to 6
- levels: int32 [8, 5], P(('copies', 'grid')), parts along dimension 0, may hold values from 1 to 3
- owner: int32 [256], P('copies'), parts along dimension 0, may hold values from 0 to 127, each once
Outputs:
- combined: float32 [256, 64, 128], P(('copies', 'grid'), 'slab'), parts along dimension 0
The draws below stay inside these ranges and needn't reach their ends.
There are 2 independent parts, one for each index of `copies`. The reference program is written for one: setup_inputs(seed, part) draws one part's arguments, and reference() takes and returns one part's arrays. A program takes and returns all parts, laid end to end along the dimension named above; each array names one. Nothing has to cross between parts.
All inputs are finite; a program needn't handle non-finite values.
Results may differ from the reference program's by a relative error of at most 0.0003.
Values sent between devices are 32-bit elements; how exact they have to be, the bound alone decides.
A program may use at most 64 MiB of HBM per device.

```python
import jax
import jax.numpy as jnp
import numpy as np
from jax import lax

N0 = 128
N1 = 2
N2 = 8
N3 = 4
N4 = 128
STEPS = 4
Q = 64
GRIDS = 4


def touch_ends(values, key, smallest, top_value):
    longest = values.shape.index(max(values.shape))
    spots = []
    for shift in (0, 1):
        where = [jax.random.randint(jax.random.fold_in(key, axis), (), 0, length) for axis, length in enumerate(values.shape)]
        where[longest] = (where[longest] + shift) % values.shape[longest]
        spots.append(tuple(where))
    return values.at[spots[0]].set(smallest).at[spots[1]].set(top_value)


def steps_of(own_key, extent, cuts, low, high):
    def one(axis_at, shards_of):
        steps = jax.random.uniform(jax.random.fold_in(jax.random.fold_in(own_key, 6), axis_at), (shards_of,), jnp.float32, low / len(cuts), high / len(cuts))
        return jnp.repeat(jnp.exp(steps), extent[axis_at] // shards_of).reshape((-1,) + (1,) * (len(extent) - axis_at - 1))

    loudness = one(*cuts[0])
    for cut in cuts[1:]:
        loudness = loudness * one(*cut)
    return loudness


def bell_draw(own_key, dims, width, most, cuts=(), held_as=jnp.bfloat16):
    loudness = steps_of(own_key, dims, cuts, -0.22, 0.18) if cuts else 1.0
    entries = jax.random.normal(own_key, dims, jnp.float32) * width * loudness
    return jnp.minimum(jnp.maximum(entries, -most), most).astype(held_as)


def setup_inputs(seed: int = 0, part: int = 0) -> dict:
    splits = jax.random.split(jax.random.key(seed), 4)
    part_splits = jax.random.split(jax.random.fold_in(splits[3], part), 4)
    return {
        "field": bell_draw(part_splits[0], (GRIDS, N0, Q, N4), 1.0, 6.0, ((0, 4), (1, 4)), jnp.float32),
        "levels": touch_ends(jax.random.randint(part_splits[1], (GRIDS, 5), 1, 4), jax.random.fold_in(part_splits[1], 1), 1, 3).astype(jnp.int32),
        "owner": jax.random.permutation(part_splits[2], N0).astype(jnp.int32),
    }


ADVECT = 0.08
DIFFUSE = 0.03

def build_tables(count):
    depth = count.bit_length() - 1
    matrix = np.eye(count)
    inverse = np.zeros((count, count))
    inverse[0, 0] = 1.0
    level_rows = np.zeros(count, np.int32)
    for index in range(1, count):
        zeros = (index & -index).bit_length() - 1
        spacing = 1 << zeros
        matrix[index, index - spacing] -= 0.5
        matrix[index, (index + spacing) % count] -= 0.5
        level_rows[index] = depth - zeros
    for zeros in range(depth - 1, -1, -1):
        spacing = 1 << zeros
        for index in range(spacing, count, 2 * spacing):
            inverse[index] = 0.5 * (inverse[index - spacing] + inverse[(index + spacing) % count])
            inverse[index, index] += 1.0
    return (matrix.astype(np.float32), inverse.astype(np.float32), level_rows)

def advance_full(state, scales):
    speed = 1.0 + 0.5 * jnp.tanh(state)
    change = jnp.zeros_like(state)
    for axis in range(5):
        back = jnp.roll(state, 1, axis)
        ahead = jnp.roll(state, -1, axis)
        change = change - ADVECT * scales[axis] * speed * (state - back) + DIFFUSE * scales[axis] ** 2 * (ahead - 2.0 * state + back)
    return state + change

def reference(field, levels, owner):
    matrix, inverse, level_rows = build_tables(N0)
    matrix = jnp.asarray(matrix).astype(jnp.float32)
    inverse = jnp.asarray(inverse).astype(jnp.float32)
    level_rows = jnp.asarray(level_rows).astype(jnp.int32)
    depth = N0.bit_length() - 1

    def keep_of(level_vec):
        return (level_rows <= depth - 3 + level_vec[0]).astype(jnp.float32)[:, None, None]

    def grid_terms(inputs):
        state, level_vec = inputs
        scales = jnp.exp2(level_vec.astype(jnp.float32)) / 8.0
        grid5 = state.reshape(N0, N1, N2, N3, N4)
        for step in range(STEPS):
            grid5 = advance_full(grid5, scales)
        hier = jnp.dot(matrix, grid5.reshape(N0, -1), precision=lax.Precision.HIGHEST).reshape(N0, Q, N4)
        weight = jnp.where(jnp.sum(level_vec) % 2 == 0, 1.0, -1.0).astype(jnp.float32) / jnp.sqrt(jnp.float32(GRIDS))
        return weight * keep_of(level_vec) * hier
    sums = lax.optimization_barrier(jnp.sum(lax.map(grid_terms, (field, levels)), axis=0))

    def restart(level_vec):
        masked = (keep_of(level_vec) * sums).reshape(N0, -1)
        return jnp.dot(inverse, masked, precision=lax.Precision.HIGHEST).reshape(N0, Q, N4)
    restarted = lax.map(restart, levels)
    sums = lax.optimization_barrier(jnp.sum(lax.map(grid_terms, (restarted, levels)), axis=0))
    return sums[owner]
```

```python
import functools
import math

import jax
import jax.numpy as jnp
from jax import lax
from jax.experimental import pallas as pl
from jax.experimental.pallas import tpu as pltpu
from jax.sharding import PartitionSpec as P

N1 = 2
N2 = 8
N3 = 4
STEPS = 4
LOW = STEPS
HIGH = STEPS + 1
EDGE = STEPS + 1
OFF = 8
RS_LAG = 1
C2_LAG = 0
SWAP_LAG = 1
PLANE_LAG = 1
CHAIN_LAG = 1

ADVECT = 0.08
DIFFUSE = 0.03
MESH = pl.DeviceIdType.MESH


def coefficients(scales, descending):
    adv = [ADVECT * x for x in scales]
    dif = [DIFFUSE * (x * x) for x in scales]
    flag = jnp.where(descending, jnp.float32(1.0), jnp.float32(0.0))
    behind, front = (1.0 - flag) * adv[0], flag * adv[0]
    return [behind, front, adv[1], adv[2], adv[3], adv[4], sum(adv[1:], adv[0]),
            dif[0], 2.0 * dif[1], dif[2], dif[3], dif[4], 1.0 - 2.0 * sum(dif[1:], dif[0])]


def advance_row(behind, u, front, coef):
    c_behind, c_front, a1, a2, a3, a4, a_sum, d0, d1, d2, d3, d4, d_own = coef
    back2 = [pltpu.roll(x, 1, 0) for x in u]
    ahead2 = [pltpu.roll(x, N2 - 1, 0) for x in u]
    back4 = [pltpu.roll(x, 1, 1) for x in u]
    ahead4 = [pltpu.roll(x, x.shape[1] - 1, 1) for x in u]
    both3 = [None] * (N1 * N3)
    for n in range(N1):
        for m in range(N3 // 2):
            pair = d3 * (u[n * N3 + m] + u[n * N3 + m + 2])
            both3[n * N3 + m + 1] = both3[n * N3 + (m + 3) % N3] = pair
    out = []
    for t in range(N1 * N3):
        n, m = divmod(t, N3)
        other = u[(N1 - 1 - n) * N3 + m]
        back3 = u[n * N3 + (m + N3 - 1) % N3]
        upwind = (c_behind * behind[t] + c_front * front[t] + a1 * other + a2 * back2[t] + a3 * back3
                  + a4 * back4[t] - a_sum * u[t])
        spread = (d0 * (behind[t] + front[t]) + d1 * other + d2 * (back2[t] + ahead2[t]) + both3[t]
                  + d4 * (back4[t] + ahead4[t]) + d_own * u[t])
        out.append(spread + (1.0 + 0.5 * jnp.tanh(u[t])) * upwind)
    return out


TILES = N1 * N3


def get(ref, *index):
    return [ref[(*index, t)] for t in range(TILES)]


def put(ref, row, *index):
    for t in range(TILES):
        ref[(*index, t)] = row[t]


def spots():
    return [pl.ds(n * N2 * N3 + m, N2, stride=N3) for n in range(N1) for m in range(N3)]


def warm_up(carry, rows, coef):
    for k in range(STEPS):
        put(carry, rows[-2], k, 0)
        put(carry, rows[-1], k, 1)
        rows = [advance_row(rows[i], rows[i + 1], rows[i + 2], coef) for i in range(len(rows) - 2)]
    put(carry, rows[-1], STEPS, 1)


def march(carry, fresh, coef):
    for k in range(STEPS):
        seq = [get(carry, k, 0), get(carry, k, 1)] + fresh
        put(carry, fresh[-2], k, 0)
        put(carry, fresh[-1], k, 1)
        fresh = [advance_row(seq[i], seq[i + 1], seq[i + 2], coef) for i in range(4)]
    old = get(carry, STEPS, 1)
    put(carry, fresh[-1], STEPS, 1)
    return [old] + fresh


def surpluses(m, first, last, mid, fine):
    coarse = [first * a + last * b for a, b in zip(m[0], m[4])]
    one = [fine * (b - 0.5 * (a + c)) for a, b, c in zip(m[0], m[1], m[2])]
    two = [mid * (b - 0.5 * (a + c)) for a, b, c in zip(m[0], m[2], m[4])]
    three = [fine * (b - 0.5 * (a + c)) for a, b, c in zip(m[2], m[3], m[4])]
    return coarse, one, two, three


def kernel(sizes, levels, owner, u_in, out, raw, carry, terms, arrived, h_terms, h_arrived, sums, carry2, part, swapped,
           fin, whole, table, lv_up, lv_down, lv_up_in, lv_down_in,
           ssem, rsem, c_send, c_recv, p_send, p_recv, x_send, x_recv, up_send, up_recv, dn_send, dn_recv,
           h_send, h_recv, in_sem):
    Z, S, rows, count, lanes = sizes
    flat = N1 * N2 * N3
    width = flat // S
    chips = S // 2
    groups = rows // 4
    owned = count // Z
    local_grids = Z // 2
    z = lax.axis_index("grid")
    s = lax.axis_index("slab")
    core = lax.rem(s, 2)
    chip = lax.div(s, 2)
    partner = s + 1 - 2 * core
    nxt, prv = lax.rem(s + 1, S), lax.rem(s + S - 1, S)
    up_z, down_z = jnp.minimum(z + 1, Z - 1), jnp.maximum(z - 1, 0)
    descending = core == 0
    to_zero = lax.rem(s + 1, 4) <= 1
    hop = jnp.where(to_zero, Z - 1 - z, z)
    h_hop = Z - 1 - hop
    main_z = jnp.where(to_zero, down_z, up_z)
    halo_z = jnp.where(to_zero, up_z, down_z)
    at_end = (z == 0) | (z == Z - 1)
    is_main = hop == Z - 1
    region = jnp.where(is_main, s, partner)
    region_desc = lax.rem(region, 2) == 0
    neighbour = jnp.where(region_desc, lax.rem(region + S - 1, S), lax.rem(region + 1, S))

    def remote(src, dst, send, recv, **where):
        return pltpu.make_async_remote_copy(src_ref=src, dst_ref=dst, send_sem=send, recv_sem=recv,
                                            device_id=where, device_id_type=MESH)

    def group_of(desc, j):
        return jnp.where(desc, groups - 1 - j, j)

    def row_of(desc, i):
        return jnp.where(desc, rows - i, i)

    loaded = pltpu.make_async_copy(u_in, raw.at[pl.ds(LOW, rows)], in_sem)
    loaded.start()
    vec = [levels[0, d] for d in range(5)]
    scales = [lax.shift_left(jnp.int32(1), v).astype(jnp.float32) * 0.125 for v in vec]
    size = jnp.float32(1.0 / math.sqrt(Z))
    weight = jnp.where(sum(vec[1:], vec[0]) % 2 == 0, size, -size)

    barrier = pltpu.get_barrier_semaphore()
    for off in range(1, S):
        pl.semaphore_signal(barrier, inc=1, device_id={"slab": lax.rem(s + off, S)}, device_id_type=MESH)

    @pl.when(z > 0)
    def _():
        pl.semaphore_signal(barrier, inc=1, device_id={"grid": down_z}, device_id_type=MESH)

    @pl.when(z < Z - 1)
    def _():
        pl.semaphore_signal(barrier, inc=1, device_id={"grid": up_z}, device_id_type=MESH)

    sub = lax.broadcasted_iota(jnp.int32, (8, lanes), 0)
    tile = jnp.zeros((8, lanes), jnp.float32)
    for d, value in enumerate(scales + [weight]):
        tile = jnp.where(sub == d, value, tile)
    for g in range(Z):
        lv_up[g] = tile
        lv_down[g] = tile
    coef = coefficients(scales, descending)
    keep_mid, keep_fine = [jnp.where(3 - t <= vec[0], jnp.float32(1.0), jnp.float32(0.0)) for t in (1, 0)]
    first_w = jnp.where(descending, 0.0 * weight, weight)
    last_w = jnp.where(descending, weight, 0.0 * weight)

    pl.semaphore_wait(barrier, S - 1 + jnp.where(z > 0, 1, 0) + jnp.where(z < Z - 1, 1, 0))

    up = remote(u_in.at[pl.ds(rows - LOW, LOW)], raw.at[pl.ds(0, LOW)], h_send.at[0], h_recv.at[0], slab=nxt)
    down = remote(u_in.at[pl.ds(0, HIGH)], raw.at[pl.ds(LOW + rows, HIGH)], h_send.at[1], h_recv.at[1], slab=prv)
    up.start()
    down.start()
    send_levels_up = remote(lv_up, lv_up_in, h_send.at[2], h_recv.at[2], grid=up_z)
    send_levels_down = remote(lv_down, lv_down_in, h_send.at[3], h_recv.at[3], grid=down_z)

    @pl.when(z == 0)
    def _():
        send_levels_up.start()

    @pl.when(z == Z - 1)
    def _():
        send_levels_down.start()

    loaded.wait()

    @pl.when(descending)
    def _():
        down.wait_recv()

    @pl.when(jnp.logical_not(descending))
    def _():
        up.wait_recv()

    def raw_row(i):
        r = LOW + row_of(descending, i)
        return [raw[r, spot] for spot in spots()]

    warm_up(carry, [raw_row(i) for i in range(-STEPS, STEPS + 1)], coef)

    def first_cycle(j):
        m = march(carry, [raw_row(4 * j + 5 + i) for i in range(4)], coef)
        r = 4 * group_of(descending, j)
        coarse, one, two, three = surpluses(m, first_w, last_w, weight * keep_mid, weight * keep_fine)
        put(terms, coarse, r)
        put(terms, one, r + jnp.where(descending, 3, 1))
        put(terms, two, r + 2)
        put(terms, three, r + jnp.where(descending, 1, 3))

    def chunk(i):
        return pl.ds(4 * group_of(descending, i), 4)

    def main_copy(i):
        return remote(terms.at[chunk(i)], arrived.at[chunk(i)], ssem.at[i], rsem.at[i], grid=main_z)

    halo_copy = remote(h_terms, h_arrived, h_send.at[4], h_recv.at[4], grid=halo_z)

    def share_copy(i):
        where = pl.ds(OFF + 4 * group_of(region_desc, i), 4)
        return remote(sums.at[where], sums.at[where], c_send.at[i], c_recv.at[i], slab=partner)

    inner_at = OFF + jnp.where(region_desc, rows, -EDGE)
    outer_at = OFF + jnp.where(region_desc, -EDGE, rows)
    inner = pl.ds(inner_at, EDGE)
    outer = pl.ds(outer_at, EDGE)
    share_inner = remote(sums.at[inner], sums.at[inner], h_send.at[5], h_recv.at[5], slab=partner)
    swap_outer = remote(sums.at[pl.ds(OFF + jnp.where(region_desc, 0, rows - EDGE), EDGE)], sums.at[inner],
                        h_send.at[6], h_recv.at[6], slab=neighbour)
    share_outer = remote(sums.at[outer], sums.at[outer], h_send.at[7], h_recv.at[7], slab=partner)

    def cell(q, keeps):
        mid_keep, fine_keep = keeps
        c = [get(sums, OFF + row_of(region_desc, 4 * q + i)) for i in range(5)]
        mid = [0.5 * (a + b) + mid_keep * x for a, b, x in zip(c[0], c[4], c[2])]
        one = [0.5 * (a + b) + fine_keep * x for a, b, x in zip(c[0], mid, c[1])]
        three = [0.5 * (a + b) + fine_keep * x for a, b, x in zip(mid, c[4], c[3])]
        return [c[0], one, mid, three, c[4]]

    NC = 13

    def build_table():
        for n in range(local_grids):
            g = n + jnp.where(is_main, 0, local_grids)
            both = jnp.where(z == 0, 1.0, 0.0) * lv_down[g] + jnp.where(z == 0, 0.0, 1.0) * lv_up[g]
            lines = [jnp.broadcast_to(both[d:d + 1], (8, lanes)) for d in range(6)]
            values = coefficients(lines[:5], region_desc)
            w = lines[5]
            mid = jnp.where(lines[0] >= 0.5, 1.0, 0.0)
            fine = jnp.where(lines[0] >= 1.0, 1.0, 0.0)
            flag = jnp.where(region_desc, 1.0, 0.0)
            values = values + [mid, fine, (1.0 - flag) * w, flag * w, mid * w, fine * w]
            for k, v in enumerate(values):
                table[n, k] = v

    def table_of(n):
        values = [table[n, k] for k in range(NC + 6)]
        return values[:NC], values[NC:NC + 2], values[NC + 2:]

    def second_warm():
        for n in range(local_grids):
            c, keeps, _ = table_of(n)
            before, after = cell(-1, keeps), cell(0, keeps)
            warm_up(carry2.at[n], before[:4] + after, c)

    def second_cycle(i):
        total = None
        for n in range(local_grids):
            c, keeps, weights = table_of(n)
            m = march(carry2.at[n], cell(i + 1, keeps)[1:], c)
            rows4 = surpluses(m, *weights)
            total = rows4 if total is None else [[a + b for a, b in zip(x, y)] for x, y in zip(total, rows4)]
        r = 4 * group_of(region_desc, i)
        places = [r, r + jnp.where(region_desc, 3, 1), r + 2, r + jnp.where(region_desc, 1, 3)]
        for place, row in zip(places, total):
            for spot, value in zip(spots(), row):
                part[place, spot] = value

    def quarter(x, c):
        return pl.ds(pl.multiple_of((2 * x + c) * width, 8), width)

    def swap_copy(i, x):
        where = pl.ds(4 * group_of(region_desc, i), 4)
        return remote(part.at[where, quarter(x, 1 - core)], swapped.at[where, x], p_send.at[i, x], p_recv.at[i, x],
                      slab=partner)

    def plane_copy(i, x):
        r = 4 * group_of(region_desc, i)
        return remote(fin.at[pl.ds(r, 4), x], whole.at[pl.ds(region * rows + r, 4)],
                      x_send.at[i, x], x_recv.at[i, chip], slab=2 * x + core)

    def slab_from(x, base):
        return 2 * x + (x % 2 if base == 0 else 1 - x % 2)

    def lot(i, x, base):
        m = slab_from(x, base)
        g = groups - 1 - i if m % 2 == 0 else i
        return pl.ds(m * rows + 4 * g, 4)

    def plane_arrival(i, x, base):
        return remote(fin.at[pl.ds(0, 4), 0], whole.at[lot(i, x, base)], x_send.at[i, x], x_recv.at[i, x],
                      slab=2 * x + core)

    def up_copy(i, x):
        return remote(whole.at[lot(i, x, 0)], whole.at[lot(i, x, 0)], up_send.at[i, x], up_recv.at[i, x], grid=up_z)

    def down_copy(i, x):
        return remote(whole.at[lot(i, x, 1)], whole.at[lot(i, x, 1)], dn_send.at[i, x], dn_recv.at[i, x],
                      grid=down_z)

    reach = (Z - 1) * RS_LAG
    start2 = reach + C2_LAG + 2
    swap_at = start2 + SWAP_LAG
    plane_at = swap_at + PLANE_LAG
    last = plane_at + (Z - 1) * CHAIN_LAG + groups

    @pl.loop(0, last)
    def _(j):
        @pl.when(j == groups - 2)
        def _():
            @pl.when(descending)
            def _():
                up.wait_recv()

            @pl.when(jnp.logical_not(descending))
            def _():
                down.wait_recv()

        @pl.when(j < groups)
        def _():
            first_cycle(j)

            @pl.when(hop == 0)
            def _():
                main_copy(j).start()

        @pl.when(j == 1)
        def _():
            e = jnp.where(descending, rows - EDGE, 0)
            for k in range(EDGE):
                put(h_terms, get(terms, e + k), k)

            @pl.when(h_hop == 0)
            def _():
                halo_copy.start()

        @pl.when((z > 0) & (j == z * RS_LAG))
        def _():
            send_levels_up.wait_recv()
            for g in range(Z):
                lv_up[g] = lv_up_in[g]
            lv_up[z] = tile

            @pl.when(z < Z - 1)
            def _():
                send_levels_up.start()

        @pl.when((z < Z - 1) & (j == (Z - 1 - z) * RS_LAG))
        def _():
            send_levels_down.wait_recv()
            for g in range(Z):
                lv_down[g] = lv_down_in[g]
            lv_down[z] = tile

            @pl.when(z > 0)
            def _():
                send_levels_down.start()

        @pl.when((h_hop > 0) & (j == 1 + h_hop * RS_LAG))
        def _():
            halo_copy.wait_recv()

            @pl.when(h_hop < Z - 1)
            def _():
                for k in range(EDGE):
                    put(h_terms, [a + b for a, b in zip(get(h_terms, k), get(h_arrived, k))], k)
                halo_copy.start()

            @pl.when(h_hop == Z - 1)
            def _():
                for k in range(EDGE):
                    put(sums, [a + b for a, b in zip(get(h_terms, k), get(h_arrived, k))], inner_at + k)
                share_inner.start()

        b = j - hop * RS_LAG

        @pl.when((hop > 0) & (b >= 0) & (b < groups))
        def _():
            main_copy(b).wait_recv()
            r = 4 * group_of(descending, b)

            @pl.when(hop < Z - 1)
            def _():
                for k in range(4):
                    put(terms, [a + c for a, c in zip(get(terms, r + k), get(arrived, r + k))], r + k)
                main_copy(b).start()

            @pl.when(hop == Z - 1)
            def _():
                for k in range(4):
                    put(sums, [a + c for a, c in zip(get(terms, r + k), get(arrived, r + k))], OFF + r + k)
                share_copy(b).start()

                @pl.when(b == groups - 1)
                def _():
                    swap_outer.start()

        i = j - start2

        @pl.when(at_end & (i == 0))
        def _():
            build_table()

            @pl.when(is_main)
            def _():
                share_inner.wait_recv()

            @pl.when(jnp.logical_not(is_main))
            def _():
                for k in range(min(2, groups)):
                    share_copy(k).wait_recv()
            second_warm()

        @pl.when(at_end & (i == groups - 2))
        def _():
            @pl.when(is_main)
            def _():
                swap_outer.wait_recv()
                share_outer.start()

            @pl.when(jnp.logical_not(is_main))
            def _():
                share_outer.wait_recv()

        @pl.when(at_end & (i >= 0) & (i < groups))
        def _():
            @pl.when(jnp.logical_not(is_main) & (i + 2 < groups))
            def _():
                share_copy(jnp.minimum(i + 2, groups - 1)).wait_recv()
            second_cycle(i)
            for x in range(chips):
                swap_copy(i, x).start()

        k = j - swap_at

        @pl.when(at_end & (k >= 0) & (k < groups))
        def _():
            r = 4 * group_of(region_desc, k)
            for x in range(chips):
                swap_copy(k, x).wait_recv()

                @pl.when(chip == x)
                def _():
                    for n in range(4):
                        whole[region * rows + r + n] = part[r + n, quarter(x, core)] + swapped[r + n, x]

                @pl.when(chip != x)
                def _():
                    for n in range(4):
                        fin[r + n, x] = part[r + n, quarter(x, core)] + swapped[r + n, x]
                    plane_copy(k, x).start()

        k2 = j - plane_at

        @pl.when((z == 0) & (k2 >= 0) & (k2 < groups))
        def _():
            for x in range(chips):
                @pl.when(chip != x)
                def _():
                    plane_arrival(k2, x, 0).wait_recv()
                up_copy(k2, x).start()

        @pl.when((z == Z - 1) & (k2 >= 0) & (k2 < groups))
        def _():
            for x in range(chips):
                @pl.when(chip != x)
                def _():
                    plane_arrival(k2, x, 1).wait_recv()
                down_copy(k2, x).start()

        f = k2 - z * CHAIN_LAG

        @pl.when((z > 0) & (f >= 0) & (f < groups))
        def _():
            for x in range(chips):
                up_copy(f, x).wait_recv()

                @pl.when(z < Z - 1)
                def _():
                    up_copy(f, x).start()

        d = k2 - (Z - 1 - z) * CHAIN_LAG

        @pl.when((z < Z - 1) & (d >= 0) & (d < groups))
        def _():
            for x in range(chips):
                down_copy(d, x).wait_recv()

                @pl.when(z > 0)
                def _():
                    down_copy(d, x).start()

    @pl.loop(0, groups)
    def _(i):
        @pl.when(hop < Z - 1)
        def _():
            main_copy(i).wait_send()

        @pl.when(at_end & is_main)
        def _():
            share_copy(i).wait_send()

        for x in range(chips):
            @pl.when(at_end)
            def _():
                swap_copy(i, x).wait_send()

            @pl.when(at_end & (chip != x))
            def _():
                plane_copy(i, x).wait_send()

            @pl.when(z < Z - 1)
            def _():
                up_copy(i, x).wait_send()

            @pl.when(z > 0)
            def _():
                down_copy(i, x).wait_send()

    up.wait_send()
    down.wait_send()

    @pl.when(h_hop < Z - 1)
    def _():
        halo_copy.wait_send()

    @pl.when(z < Z - 1)
    def _():
        send_levels_up.wait_send()

    @pl.when(z > 0)
    def _():
        send_levels_down.wait_send()

    @pl.when(at_end & is_main)
    def _():
        swap_outer.wait_send()
        share_outer.wait_send()

    @pl.when(at_end & jnp.logical_not(is_main))
    def _():
        share_inner.wait_send()

    for spacing in [1 << t for t in range(2, count.bit_length() - 1)]:
        for i in range(spacing, count, 2 * spacing):
            whole[i] = whole[i] - 0.5 * (whole[i - spacing] + whole[(i + spacing) % count])

    @pl.loop(0, owned)
    def _(r):
        out[r] = whole[owner[z * owned + r]]


def local(field, levels, owner):
    _, rows, flat, lanes = field.shape
    Z, S = lax.axis_size("grid"), lax.axis_size("slab")
    count = owner.shape[0]
    width = flat // S
    owned = count // Z
    groups = rows // 4
    chips = S // 2
    grids = Z // 2
    tail = (TILES, N2, lanes)
    vmem = lambda *shape: pltpu.VMEM(shape, jnp.float32)
    sems = lambda *shape: pltpu.SemaphoreType.DMA(shape)
    level_tiles = vmem(Z, 8, lanes)
    return pl.pallas_call(
        functools.partial(kernel, (Z, S, rows, count, lanes)),
        out_shape=jax.ShapeDtypeStruct((owned, width, lanes), jnp.float32),
        in_specs=[pl.BlockSpec(memory_space=pltpu.SMEM), pl.BlockSpec(memory_space=pltpu.SMEM),
                  pl.BlockSpec(memory_space=pl.ANY)],
        out_specs=pl.BlockSpec(memory_space=pltpu.VMEM),
        scratch_shapes=[
            vmem(rows + LOW + HIGH, flat, lanes), vmem(STEPS + 1, 2, *tail), vmem(rows, *tail), vmem(rows, *tail),
            vmem(EDGE, *tail), vmem(EDGE, *tail), vmem(OFF + rows + EDGE, *tail),
            vmem(grids, STEPS + 1, 2, *tail), vmem(rows, flat, lanes), vmem(rows, chips, width, lanes),
            vmem(rows, chips, width, lanes), vmem(count, width, lanes), vmem(grids, 19, 8, lanes),
            level_tiles, level_tiles, level_tiles, level_tiles,
            sems(groups), sems(groups), sems(groups), sems(groups), sems(groups, chips), sems(groups, chips),
            sems(groups, chips), sems(groups, chips), sems(groups, chips), sems(groups, chips),
            sems(groups, chips), sems(groups, chips), sems(8), sems(8), pltpu.SemaphoreType.DMA,
        ],
        compiler_params=pltpu.CompilerParams(collective_id=0, has_side_effects=True,
                                             vmem_limit_bytes=40 * 1024 * 1024),
    )(levels, owner, field[0])


def solution(mesh):
    in_specs = (P(("copies", "grid"), "slab", None, None), P(("copies", "grid"), None), P("copies"))
    out_specs = P(("copies", "grid"), "slab", None)
    return jax.shard_map(local, mesh=mesh, in_specs=in_specs, out_specs=out_specs, check_vma=False)
```

```python
import functools
import math

import jax
import jax.numpy as jnp
from jax import lax
from jax.experimental import pallas as pl
from jax.experimental.pallas import tpu as pltpu
from jax.sharding import PartitionSpec as P

N1 = 2
N2 = 8
N3 = 4
STEPS = 4
EDGE = STEPS + 1
WIDE = 2 * STEPS + 1
OFF = 8
PIECE = 2
DIRECT = 8
RS_LAG = 2
C2_LAG = 1
SWAP_LAG = 1
PLANE_LAG = 2
CHAIN_LAG = 2

ADVECT = 0.08
DIFFUSE = 0.03
MESH = pl.DeviceIdType.MESH


def coefficients(scales, descending):
    adv = [ADVECT * x for x in scales]
    dif = [DIFFUSE * (x * x) for x in scales]
    flag = jnp.where(descending, jnp.float32(1.0), jnp.float32(0.0))
    behind, front = (1.0 - flag) * adv[0], flag * adv[0]
    return [behind, front, adv[1], adv[2], adv[3], adv[4], sum(adv[1:], adv[0]),
            dif[0], 2.0 * dif[1], dif[2], dif[3], dif[4], 1.0 - 2.0 * sum(dif[1:], dif[0])]


def advance_row(behind, u, front, coef):
    c_behind, c_front, a1, a2, a3, a4, a_sum, d0, d1, d2, d3, d4, d_own = coef
    back2 = [pltpu.roll(x, 1, 0) for x in u]
    ahead2 = [pltpu.roll(x, N2 - 1, 0) for x in u]
    back4 = [pltpu.roll(x, 1, 1) for x in u]
    ahead4 = [pltpu.roll(x, x.shape[1] - 1, 1) for x in u]
    both3 = [None] * (N1 * N3)
    for n in range(N1):
        for m in range(N3 // 2):
            pair = d3 * (u[n * N3 + m] + u[n * N3 + m + 2])
            both3[n * N3 + m + 1] = both3[n * N3 + (m + 3) % N3] = pair
    out = []
    for t in range(N1 * N3):
        n, m = divmod(t, N3)
        other = u[(N1 - 1 - n) * N3 + m]
        back3 = u[n * N3 + (m + N3 - 1) % N3]
        upwind = (c_behind * behind[t] + c_front * front[t] + a1 * other + a2 * back2[t] + a3 * back3
                  + a4 * back4[t] - a_sum * u[t])
        spread = (d0 * (behind[t] + front[t]) + d1 * other + d2 * (back2[t] + ahead2[t]) + both3[t]
                  + d4 * (back4[t] + ahead4[t]) + d_own * u[t])
        out.append(spread + (1.0 + 0.5 * jnp.tanh(u[t])) * upwind)
    return out


TILES = N1 * N3


def get(ref, *index):
    return [ref[(*index, t)] for t in range(TILES)]


def put(ref, row, *index):
    for t in range(TILES):
        ref[(*index, t)] = row[t]


def spots():
    return [pl.ds(n * N2 * N3 + m, N2, stride=N3) for n in range(N1) for m in range(N3)]


def warm_up(carry, rows, coef):
    for k in range(STEPS):
        put(carry, rows[-2], k, 0)
        put(carry, rows[-1], k, 1)
        rows = [advance_row(rows[i], rows[i + 1], rows[i + 2], coef) for i in range(len(rows) - 2)]
    put(carry, rows[-1], STEPS, 1)


def march(carry, fresh, coef):
    for k in range(STEPS):
        seq = [get(carry, k, 0), get(carry, k, 1)] + fresh
        put(carry, fresh[-2], k, 0)
        put(carry, fresh[-1], k, 1)
        fresh = [advance_row(seq[i], seq[i + 1], seq[i + 2], coef) for i in range(4)]
    old = get(carry, STEPS, 1)
    put(carry, fresh[-1], STEPS, 1)
    return [old] + fresh


def surpluses(m, first, last, mid, fine):
    coarse = [first * a + last * b for a, b in zip(m[0], m[4])]
    one = [fine * (b - 0.5 * (a + c)) for a, b, c in zip(m[0], m[1], m[2])]
    two = [mid * (b - 0.5 * (a + c)) for a, b, c in zip(m[0], m[2], m[4])]
    three = [fine * (b - 0.5 * (a + c)) for a, b, c in zip(m[2], m[3], m[4])]
    return coarse, one, two, three


def kernel(sizes, levels_in, owner_in, u_in, out, levels, owner, raw, carry, terms, arrived, h_out, h_terms, h_arrived, o_terms, o_arrived,
           sums, carry2, part, swapped, fin, whole, coarse, table, lv, lv_in,
           ssem, rsem, c_send, c_recv, p_send, p_recv, x_send, x_recv, up_send, up_recv, dn_send, dn_recv, all_send,
           h_send, h_recv, in_sem):
    Z, S, rows, count, lanes = sizes
    flat = N1 * N2 * N3
    width = flat // S
    chips = S // 2
    groups = rows // 4
    owned = count // Z
    local_grids = Z // 2
    z = lax.axis_index("grid")
    s = lax.axis_index("slab")
    core = lax.rem(s, 2)
    chip = lax.div(s, 2)
    partner = s + 1 - 2 * core
    nxt, prv = lax.rem(s + 1, S), lax.rem(s + S - 1, S)
    up_z, down_z = jnp.minimum(z + 1, Z - 1), jnp.maximum(z - 1, 0)
    descending = core == 0
    to_zero = lax.rem(s + 1, 4) <= 1
    hop = jnp.where(to_zero, Z - 1 - z, z)
    main_z = jnp.where(to_zero, down_z, up_z)
    at_end = (z == 0) | (z == Z - 1)
    is_main = hop == Z - 1
    region = jnp.where(is_main, s, partner)
    region_desc = lax.rem(region, 2) == 0
    neighbour = jnp.where(descending, prv, nxt)
    direct_from = min(DIRECT, groups)

    def remote(src, dst, send, recv, **where):
        return pltpu.make_async_remote_copy(src_ref=src, dst_ref=dst, send_sem=send, recv_sem=recv,
                                            device_id=where, device_id_type=MESH)

    def group_of(desc, j):
        return jnp.where(desc, groups - 1 - j, j)

    def row_of(desc, i):
        return jnp.where(desc, rows - i, i)

    small = pltpu.make_async_copy(levels_in, levels, in_sem.at[1])
    small.start()
    loaded = pltpu.make_async_copy(u_in, raw.at[pl.ds(WIDE, rows)], in_sem.at[0])
    loaded.start()
    owners = pltpu.make_async_copy(owner_in, owner, in_sem.at[2])
    owners.start()
    barrier = pltpu.get_barrier_semaphore()
    for off in range(1, S):
        pl.semaphore_signal(barrier, inc=1, device_id={"slab": lax.rem(s + off, S)}, device_id_type=MESH)

    @pl.when(z > 0)
    def _():
        pl.semaphore_signal(barrier, inc=1, device_id={"grid": down_z}, device_id_type=MESH)

    @pl.when(z < Z - 1)
    def _():
        pl.semaphore_signal(barrier, inc=1, device_id={"grid": up_z}, device_id_type=MESH)

    small.wait()
    vec = [levels[0, d] for d in range(5)]
    scales = [lax.shift_left(jnp.int32(1), v).astype(jnp.float32) * 0.125 for v in vec]
    size = jnp.float32(1.0 / math.sqrt(Z))
    weight = jnp.where(sum(vec[1:], vec[0]) % 2 == 0, size, -size)

    sub = lax.broadcasted_iota(jnp.int32, (8, lanes), 0)
    tile = jnp.zeros((8, lanes), jnp.float32)
    for d, value in enumerate(scales + [weight]):
        tile = jnp.where(sub == d, value, tile)
    for g in range(Z):
        lv[g] = tile
    coef = coefficients(scales, descending)
    keep_mid, keep_fine = [jnp.where(3 - t <= vec[0], jnp.float32(1.0), jnp.float32(0.0)) for t in (1, 0)]
    first_w = jnp.where(descending, 0.0 * weight, weight)
    last_w = jnp.where(descending, weight, 0.0 * weight)

    pl.semaphore_wait(barrier, S - 1 + jnp.where(z > 0, 1, 0) + jnp.where(z < Z - 1, 1, 0))

    inner_halo = remote(u_in.at[pl.ds(jnp.where(descending, rows - EDGE, 0), EDGE)],
                        raw.at[pl.ds(jnp.where(descending, WIDE - EDGE, WIDE + rows), EDGE)],
                        h_send.at[0], h_recv.at[0], slab=partner)
    outer_halo = remote(u_in.at[pl.ds(jnp.where(descending, 0, rows - WIDE), WIDE)],
                        raw.at[pl.ds(jnp.where(descending, WIDE + rows, 0), WIDE)],
                        h_send.at[1], h_recv.at[1], slab=neighbour)
    inner_halo.start()
    outer_halo.start()
    send_levels = remote(lv, lv_in, h_send.at[2], h_recv.at[2], grid=main_z)
    share_levels = remote(lv, lv_in, h_send.at[3], h_recv.at[3], slab=partner)

    @pl.when(hop == 0)
    def _():
        send_levels.start()

    loaded.wait()

    inner_halo.wait_recv()

    def raw_row(i):
        r = WIDE + row_of(descending, i)
        return [raw[r, spot] for spot in spots()]

    warm_up(carry, [raw_row(i) for i in range(-STEPS, STEPS + 1)], coef)

    def first_cycle(j):
        m = march(carry, [raw_row(4 * j + 5 + i) for i in range(4)], coef)
        four = surpluses(m, first_w, last_w, weight * keep_mid, weight * keep_fine)
        order = [0, jnp.where(descending, 3, 1), 2, jnp.where(descending, 1, 3)]

        @pl.when(j < groups)
        def _():
            for k, row in zip(order, four):
                put(terms, row, 4 * group_of(descending, j) + k)

        @pl.when(j == groups)
        def _():
            for k, row in zip(order, four):
                put(o_terms, row, k + jnp.where(descending, 1, 0))
            put(o_terms, [weight * x for x in m[4]], jnp.where(descending, 0, 4))

    def piece(i, h):
        return pl.ds(4 * group_of(descending, i) + PIECE * h, PIECE)

    def main_copy(i, h):
        return remote(terms.at[piece(i, h)], arrived.at[piece(i, h)], ssem.at[i, h], rsem.at[i, h], grid=main_z)

    halo_copy = remote(h_terms, h_arrived, h_send.at[4], h_recv.at[4], grid=main_z)
    halo_swap = remote(h_out, h_terms, h_send.at[8], h_recv.at[8], slab=partner)
    outer_copy = remote(o_terms, o_arrived, h_send.at[6], h_recv.at[6], grid=main_z)

    def share_copy(i):
        where = pl.ds(OFF + 4 * group_of(region_desc, i), 4)
        return remote(sums.at[where], sums.at[where], c_send.at[i], c_recv.at[i], slab=partner)

    inner_at = OFF + jnp.where(region_desc, rows, -EDGE)
    outer_at = OFF + jnp.where(region_desc, -EDGE, rows)
    inner = pl.ds(inner_at, EDGE)
    outer = pl.ds(outer_at, EDGE)
    share_inner = remote(sums.at[inner], sums.at[inner], h_send.at[5], h_recv.at[5], slab=partner)
    share_outer = remote(sums.at[outer], sums.at[outer], h_send.at[7], h_recv.at[7], slab=partner)

    def cell(q, keeps):
        mid_keep, fine_keep = keeps
        c = [get(sums, OFF + row_of(region_desc, 4 * q + i)) for i in range(5)]
        mid = [0.5 * (a + b) + mid_keep * x for a, b, x in zip(c[0], c[4], c[2])]
        one = [0.5 * (a + b) + fine_keep * x for a, b, x in zip(c[0], mid, c[1])]
        three = [0.5 * (a + b) + fine_keep * x for a, b, x in zip(mid, c[4], c[3])]
        return [c[0], one, mid, three, c[4]]

    NC = 13

    def build_table():
        for n in range(local_grids):
            g = n + jnp.where(is_main, 0, local_grids)
            both = jnp.where(is_main, 1.0, 0.0) * lv[g] + jnp.where(is_main, 0.0, 1.0) * lv_in[g]
            lines = [jnp.broadcast_to(both[d:d + 1], (8, lanes)) for d in range(6)]
            values = coefficients(lines[:5], region_desc)
            w = lines[5]
            mid = jnp.where(lines[0] >= 0.5, 1.0, 0.0)
            fine = jnp.where(lines[0] >= 1.0, 1.0, 0.0)
            flag = jnp.where(region_desc, 1.0, 0.0)
            values = values + [mid, fine, (1.0 - flag) * w, flag * w, mid * w, fine * w]
            for k, v in enumerate(values):
                table[n, k] = v

    def table_of(n):
        values = [table[n, k] for k in range(NC + 6)]
        return values[:NC], values[NC:NC + 2], values[NC + 2:]

    def second_warm():
        for n in range(local_grids):
            c, keeps, _ = table_of(n)
            before, after = cell(-1, keeps), cell(0, keeps)
            warm_up(carry2.at[n], before[:4] + after, c)

    def second_cycle(i):
        total = None
        for n in range(local_grids):
            c, keeps, weights = table_of(n)
            m = march(carry2.at[n], cell(i + 1, keeps)[1:], c)
            rows4 = surpluses(m, *weights)
            total = rows4 if total is None else [[a + b for a, b in zip(x, y)] for x, y in zip(total, rows4)]
        r = 4 * group_of(region_desc, i)
        places = [r, r + jnp.where(region_desc, 3, 1), r + 2, r + jnp.where(region_desc, 1, 3)]
        for place, row in zip(places, total):
            for spot, value in zip(spots(), row):
                part[place, spot] = value

    def quarter(x, c):
        return pl.ds(pl.multiple_of((2 * x + c) * width, 8), width)

    def swap_copy(i, x):
        where = pl.ds(4 * group_of(region_desc, i), 4)
        return remote(part.at[where, quarter(x, 1 - core)], swapped.at[where, x], p_send.at[i, x], p_recv.at[i, x],
                      slab=partner)

    def plane_copy(i, x):
        r = 4 * group_of(region_desc, i)
        return remote(fin.at[pl.ds(r, 4), x], whole.at[pl.ds(region * rows + r, 4)],
                      x_send.at[i, x], x_recv.at[i, chip], slab=2 * x + core)

    def direct_copy(i, x, to, own, recv):
        r = 4 * group_of(region_desc, i)
        here = whole.at[pl.ds(region * rows + r, 4)]
        return remote(here if own else fin.at[pl.ds(r, 4), x], here, all_send.at[i, x, to], recv.at[i, chip],
                      grid=to, slab=2 * x + core)

    def slab_from(x, base):
        return 2 * x + (x % 2 if base == 0 else 1 - x % 2)

    def lot(i, x, base):
        m = slab_from(x, base)
        g = groups - 1 - i if m % 2 == 0 else i
        return pl.ds(m * rows + 4 * g, 4)

    def plane_arrival(i, x, base):
        return remote(fin.at[pl.ds(0, 4), 0], whole.at[lot(i, x, base)], x_send.at[i, x], x_recv.at[i, x],
                      slab=2 * x + core)

    def up_copy(i, x):
        return remote(whole.at[lot(i, x, 0)], whole.at[lot(i, x, 0)], up_send.at[i, x], up_recv.at[i, x], grid=up_z)

    def down_copy(i, x):
        return remote(whole.at[lot(i, x, 1)], whole.at[lot(i, x, 1)], dn_send.at[i, x], dn_recv.at[i, x],
                      grid=down_z)

    reach = (Z - 1) * RS_LAG
    start2 = reach + C2_LAG + 2
    swap_at = start2 + SWAP_LAG
    plane_at = swap_at + PLANE_LAG
    last = max(swap_at + groups, plane_at + (Z - 2) * CHAIN_LAG + direct_from, plane_at + direct_from)

    @pl.loop(0, last)
    def _(j):
        @pl.when(j == groups - 2)
        def _():
            outer_halo.wait_recv()

        @pl.when((hop == 0) & (j == 2))
        def _():
            halo_swap.wait_recv()
            halo_copy.start()

        @pl.when(j <= groups)
        def _():
            first_cycle(j)

            @pl.when((hop == 0) & (j < groups))
            def _():
                for h in range(4 // PIECE):
                    main_copy(j, h).start()

        @pl.when((hop == 0) & (j == groups))
        def _():
            outer_copy.start()

        @pl.when(j == 1)
        def _():
            e = jnp.where(descending, rows - EDGE, 0)
            for k in range(EDGE):
                put(h_out, get(terms, e + k), k)
            halo_swap.start()

        @pl.when((hop > 0) & (j == hop * RS_LAG))
        def _():
            send_levels.wait_recv()
            for g in range(Z):
                lv[g] = lv_in[g]
            lv[z] = tile

            @pl.when(hop < Z - 1)
            def _():
                send_levels.start()

            @pl.when(hop == Z - 1)
            def _():
                share_levels.start()

        b = j - hop * RS_LAG

        @pl.when((hop > 0) & (b == 2))
        def _():
            halo_swap.wait_recv()
            halo_copy.wait_recv()

            @pl.when(hop < Z - 1)
            def _():
                for k in range(EDGE):
                    put(h_terms, [a + b for a, b in zip(get(h_terms, k), get(h_arrived, k))], k)
                halo_copy.start()

            @pl.when(hop == Z - 1)
            def _():
                for k in range(EDGE):
                    put(sums, [a + b for a, b in zip(get(h_terms, k), get(h_arrived, k))], inner_at + k)
                share_inner.start()

        @pl.when((hop > 0) & (b >= 0) & (b < groups))
        def _():
            @pl.when(hop < Z - 1)
            def _():
                for h in range(4 // PIECE):
                    r = 4 * group_of(descending, b) + h * PIECE
                    main_copy(b, h).wait_recv()
                    for k in range(PIECE):
                        put(terms, [a + c for a, c in zip(get(terms, r + k), get(arrived, r + k))], r + k)
                    main_copy(b, h).start()

            @pl.when(hop == Z - 1)
            def _():
                for h in range(4 // PIECE):
                    r = 4 * group_of(descending, b) + h * PIECE
                    main_copy(b, h).wait_recv()
                    for k in range(PIECE):
                        put(sums, [a + c for a, c in zip(get(terms, r + k), get(arrived, r + k))], OFF + r + k)
                share_copy(b).start()

        @pl.when((hop > 0) & (b == groups))
        def _():
            outer_copy.wait_recv()

            @pl.when(hop < Z - 1)
            def _():
                for k in range(EDGE):
                    put(o_terms, [a + c for a, c in zip(get(o_terms, k), get(o_arrived, k))], k)
                outer_copy.start()

            @pl.when(hop == Z - 1)
            def _():
                for k in range(EDGE):
                    put(sums, [a + c for a, c in zip(get(o_terms, k), get(o_arrived, k))], outer_at + k)
                share_outer.start()

        i = j - start2

        @pl.when(at_end & (i == 0))
        def _():
            @pl.when(jnp.logical_not(is_main))
            def _():
                share_levels.wait_recv()
                share_inner.wait_recv()
                for k in range(min(2, groups)):
                    share_copy(k).wait_recv()
            build_table()
            second_warm()

        @pl.when(at_end & jnp.logical_not(is_main) & (i == groups - 2))
        def _():
            share_outer.wait_recv()

        @pl.when(at_end & (i >= 0) & (i < groups))
        def _():
            @pl.when(jnp.logical_not(is_main) & (i + 2 < groups))
            def _():
                share_copy(jnp.minimum(i + 2, groups - 1)).wait_recv()
            second_cycle(i)
            for x in range(chips):
                swap_copy(i, x).start()

        k = j - swap_at

        @pl.when(at_end & (k >= 0) & (k < groups))
        def _():
            r = 4 * group_of(region_desc, k)
            for x in range(chips):
                swap_copy(k, x).wait_recv()

                @pl.when(chip == x)
                def _():
                    for n in range(4):
                        whole[region * rows + r + n] = part[r + n, quarter(x, core)] + swapped[r + n, x]

                @pl.when(chip != x)
                def _():
                    for n in range(4):
                        fin[r + n, x] = part[r + n, quarter(x, core)] + swapped[r + n, x]
                    plane_copy(k, x).start()

            @pl.when(k >= direct_from)
            def _():
                @pl.loop(1, Z)
                def _(away):
                    for x in range(chips):
                        to = jnp.where(z == 0, Z - away, away - 1)

                        @pl.when((z == 0) & (chip == x))
                        def _():
                            direct_copy(k, x, to, True, up_recv).start()

                        @pl.when((z == 0) & (chip != x))
                        def _():
                            direct_copy(k, x, to, False, up_recv).start()

                        @pl.when((z > 0) & (chip == x))
                        def _():
                            direct_copy(k, x, to, True, dn_recv).start()

                        @pl.when((z > 0) & (chip != x))
                        def _():
                            direct_copy(k, x, to, False, dn_recv).start()

        k2 = j - plane_at

        @pl.when((z == 0) & (k2 >= 0) & (k2 < direct_from))
        def _():
            for x in range(chips):
                @pl.when(chip != x)
                def _():
                    plane_arrival(k2, x, 0).wait_recv()
                up_copy(k2, x).start()

        @pl.when((z == Z - 1) & (k2 >= 0) & (k2 < direct_from))
        def _():
            for x in range(chips):
                @pl.when(chip != x)
                def _():
                    plane_arrival(k2, x, 1).wait_recv()
                down_copy(k2, x).start()

        f = k2 - z * CHAIN_LAG

        @pl.when((z > 0) & (z < Z - 1) & (f >= 0) & (f < direct_from))
        def _():
            for x in range(chips):
                up_copy(f, x).wait_recv()
                up_copy(f, x).start()

        d = k2 - (Z - 1 - z) * CHAIN_LAG

        @pl.when((z < Z - 1) & (z > 0) & (d >= 0) & (d < direct_from))
        def _():
            for x in range(chips):
                down_copy(d, x).wait_recv()
                down_copy(d, x).start()

    @pl.loop(0, groups)
    def _(i):
        for x in range(chips):
            @pl.when((z == Z - 1) | ((z > 0) & (i >= direct_from)))
            def _():
                up_copy(i, x).wait_recv()

            @pl.when((z == 0) | ((z < Z - 1) & (i >= direct_from)))
            def _():
                down_copy(i, x).wait_recv()

            @pl.when((z == 0) & (chip != x) & (i >= direct_from))
            def _():
                plane_arrival(i, x, 0).wait_recv()

            @pl.when((z == Z - 1) & (chip != x) & (i >= direct_from))
            def _():
                plane_arrival(i, x, 1).wait_recv()

    owners.wait()

    def nodal(i):
        return coarse[i // 4]

    for i in range(0, count, 4):
        coarse[i // 4] = whole[i]
    for spacing in [1 << t for t in range(2, count.bit_length() - 1)]:
        for i in range(spacing, count, 2 * spacing):
            coarse[i // 4] = nodal(i) - 0.5 * (nodal(i - spacing) + nodal((i + spacing) % count))

    for r in range(owned):
        position = owner[z * owned + r]
        top = jnp.where(position % 4 == 0, jnp.float32(1.0), jnp.float32(0.0))
        out[r] = top * coarse[position // 4] + (1.0 - top) * whole[position]

    @pl.loop(0, groups)
    def _(i):
        @pl.when(hop < Z - 1)
        def _():
            for h in range(4 // PIECE):
                main_copy(i, h).wait_send()

        @pl.when(at_end & is_main)
        def _():
            share_copy(i).wait_send()

        for x in range(chips):
            @pl.when(at_end)
            def _():
                swap_copy(i, x).wait_send()

            @pl.when(at_end & (chip != x))
            def _():
                plane_copy(i, x).wait_send()

            @pl.when((z < Z - 1) & (i < direct_from))
            def _():
                up_copy(i, x).wait_send()

            @pl.when((z > 0) & (i < direct_from))
            def _():
                down_copy(i, x).wait_send()

            @pl.when(at_end & (i >= direct_from))
            def _():
                @pl.loop(1, Z)
                def _(away):
                    to = jnp.where(z == 0, Z - away, away - 1)
                    direct_copy(i, x, to, False, up_recv).wait_send()

    inner_halo.wait_send()
    outer_halo.wait_send()
    halo_swap.wait_send()

    @pl.when(hop < Z - 1)
    def _():
        halo_copy.wait_send()
        outer_copy.wait_send()
        send_levels.wait_send()

    @pl.when(at_end & is_main)
    def _():
        share_levels.wait_send()
        share_inner.wait_send()
        share_outer.wait_send()


def local(field, levels, owner):
    _, rows, flat, lanes = field.shape
    Z, S = lax.axis_size("grid"), lax.axis_size("slab")
    count = owner.shape[0]
    width = flat // S
    owned = count // Z
    groups = rows // 4
    chips = S // 2
    grids = Z // 2
    tail = (TILES, N2, lanes)
    vmem = lambda *shape: pltpu.VMEM(shape, jnp.float32)
    sems = lambda *shape: pltpu.SemaphoreType.DMA(shape)
    level_tiles = vmem(Z, 8, lanes)
    hbm = pl.BlockSpec(memory_space=pltpu.HBM)
    return pl.pallas_call(
        functools.partial(kernel, (Z, S, rows, count, lanes)),
        out_shape=jax.ShapeDtypeStruct((owned, width, lanes), jnp.float32),
        in_specs=[hbm, hbm, hbm],
        out_specs=pl.BlockSpec(memory_space=pltpu.VMEM),
        scratch_shapes=[
            pltpu.SMEM(levels.shape, jnp.int32), pltpu.SMEM(owner.shape, jnp.int32),
            vmem(rows + 2 * WIDE, flat, lanes), vmem(STEPS + 1, 2, *tail), vmem(rows, *tail), vmem(rows, *tail),
            vmem(EDGE, *tail), vmem(EDGE, *tail), vmem(EDGE, *tail),
            vmem(EDGE, *tail), vmem(EDGE, *tail), vmem(OFF + rows + EDGE, *tail),
            vmem(grids, STEPS + 1, 2, *tail), vmem(rows, flat, lanes), vmem(rows, chips, width, lanes),
            vmem(rows, chips, width, lanes), vmem(count, width, lanes), vmem(count // 4, width, lanes),
            vmem(grids, 19, 8, lanes), level_tiles, level_tiles,
            sems(groups, 4 // PIECE), sems(groups, 4 // PIECE), sems(groups), sems(groups),
            sems(groups, chips), sems(groups, chips), sems(groups, chips), sems(groups, chips),
            sems(groups, chips), sems(groups, chips), sems(groups, chips), sems(groups, chips),
            sems(groups, chips, Z), sems(10), sems(10), sems(3),
        ],
        compiler_params=pltpu.CompilerParams(collective_id=0, has_side_effects=True,
                                             vmem_limit_bytes=40 * 1024 * 1024),
    )(levels, owner, field[0])


def solution(mesh):
    in_specs = (P(("copies", "grid"), "slab", None, None), P(("copies", "grid"), None), P("copies"))
    out_specs = P(("copies", "grid"), "slab", None)
    return jax.shard_map(local, mesh=mesh, in_specs=in_specs, out_specs=out_specs, check_vma=False)
```

```python
import functools
import math

import jax
import jax.numpy as jnp
from jax import lax
from jax.experimental import pallas as pl
from jax.experimental.pallas import tpu as pltpu
from jax.sharding import PartitionSpec as P

N1 = 2
N2 = 8
N3 = 4
STEPS = 4
EDGE = STEPS + 1
WIDE = 2 * STEPS + 1
OFF = 8
PIECE = 2
DIRECT = 8
RS_LAG = 2
C2_LAG = 1
SWAP_LAG = 1
PLANE_LAG = 2
CHAIN_LAG = 2

ADVECT = 0.08
DIFFUSE = 0.03
MESH = pl.DeviceIdType.MESH


def coefficients(scales, descending):
    adv = [ADVECT * x for x in scales]
    dif = [DIFFUSE * (x * x) for x in scales]
    flag = jnp.where(descending, jnp.float32(1.0), jnp.float32(0.0))
    behind, front = (1.0 - flag) * adv[0], flag * adv[0]
    return [behind, front, adv[1], adv[2], adv[3], adv[4], sum(adv[1:], adv[0]),
            dif[0], 2.0 * dif[1], dif[2], dif[3], dif[4], 1.0 - 2.0 * sum(dif[1:], dif[0])]


def advance_row(behind, u, front, coef):
    c_behind, c_front, a1, a2, a3, a4, a_sum, d0, d1, d2, d3, d4, d_own = coef
    back2 = [pltpu.roll(x, 1, 0) for x in u]
    ahead2 = [pltpu.roll(x, N2 - 1, 0) for x in u]
    back4 = [pltpu.roll(x, 1, 1) for x in u]
    ahead4 = [pltpu.roll(x, x.shape[1] - 1, 1) for x in u]
    both3 = [None] * (N1 * N3)
    for n in range(N1):
        for m in range(N3 // 2):
            pair = d3 * (u[n * N3 + m] + u[n * N3 + m + 2])
            both3[n * N3 + m + 1] = both3[n * N3 + (m + 3) % N3] = pair
    out = []
    for t in range(N1 * N3):
        n, m = divmod(t, N3)
        other = u[(N1 - 1 - n) * N3 + m]
        back3 = u[n * N3 + (m + N3 - 1) % N3]
        upwind = (c_behind * behind[t] + c_front * front[t] + a1 * other + a2 * back2[t] + a3 * back3
                  + a4 * back4[t] - a_sum * u[t])
        spread = (d0 * (behind[t] + front[t]) + d1 * other + d2 * (back2[t] + ahead2[t]) + both3[t]
                  + d4 * (back4[t] + ahead4[t]) + d_own * u[t])
        out.append(spread + (1.0 + 0.5 * jnp.tanh(u[t])) * upwind)
    return out


TILES = N1 * N3


def get(ref, *index):
    return [ref[(*index, t)] for t in range(TILES)]


def put(ref, row, *index):
    for t in range(TILES):
        ref[(*index, t)] = row[t]


def spots():
    return [pl.ds(n * N2 * N3 + m, N2, stride=N3) for n in range(N1) for m in range(N3)]


def warm_up(carry, rows, coef):
    for k in range(STEPS):
        put(carry, rows[-2], k, 0)
        put(carry, rows[-1], k, 1)
        rows = [advance_row(rows[i], rows[i + 1], rows[i + 2], coef) for i in range(len(rows) - 2)]
    put(carry, rows[-1], STEPS, 1)


def march(carry, fresh, coef):
    for k in range(STEPS):
        seq = [get(carry, k, 0), get(carry, k, 1)] + fresh
        put(carry, fresh[-2], k, 0)
        put(carry, fresh[-1], k, 1)
        fresh = [advance_row(seq[i], seq[i + 1], seq[i + 2], coef) for i in range(4)]
    old = get(carry, STEPS, 1)
    put(carry, fresh[-1], STEPS, 1)
    return [old] + fresh


def surpluses(m, first, last, mid, fine):
    coarse = [first * a + last * b for a, b in zip(m[0], m[4])]
    one = [fine * (b - 0.5 * (a + c)) for a, b, c in zip(m[0], m[1], m[2])]
    two = [mid * (b - 0.5 * (a + c)) for a, b, c in zip(m[0], m[2], m[4])]
    three = [fine * (b - 0.5 * (a + c)) for a, b, c in zip(m[2], m[3], m[4])]
    return coarse, one, two, three


def kernel(sizes, levels_in, owner_in, u_in, out, levels, owner, raw, carry, terms, arrived, h_out, h_terms, h_arrived, o_terms, o_arrived,
           sums, carry2, part, swapped, fin, whole, coarse, table, lv, lv_in,
           ssem, rsem, c_send, c_recv, p_send, p_recv, x_send, x_recv, up_send, up_recv, dn_send, dn_recv, all_send, e_send, e_recv,
           h_send, h_recv, in_sem):
    Z, S, rows, count, lanes = sizes
    flat = N1 * N2 * N3
    width = flat // S
    chips = S // 2
    groups = rows // 4
    owned = count // Z
    local_grids = Z // 2
    z = lax.axis_index("grid")
    s = lax.axis_index("slab")
    core = lax.rem(s, 2)
    chip = lax.div(s, 2)
    partner = s + 1 - 2 * core
    nxt, prv = lax.rem(s + 1, S), lax.rem(s + S - 1, S)
    up_z, down_z = jnp.minimum(z + 1, Z - 1), jnp.maximum(z - 1, 0)
    descending = core == 0
    to_zero = lax.rem(s + 1, 4) <= 1
    hop = jnp.where(to_zero, Z - 1 - z, z)
    main_z = jnp.where(to_zero, down_z, up_z)
    at_end = (z == 0) | (z == Z - 1)
    is_main = hop == Z - 1
    region = jnp.where(is_main, s, partner)
    region_desc = lax.rem(region, 2) == 0
    neighbour = jnp.where(descending, prv, nxt)
    direct_from = min(DIRECT, groups)

    def remote(src, dst, send, recv, **where):
        return pltpu.make_async_remote_copy(src_ref=src, dst_ref=dst, send_sem=send, recv_sem=recv,
                                            device_id=where, device_id_type=MESH)

    def group_of(desc, j):
        return jnp.where(desc, groups - 1 - j, j)

    def row_of(desc, i):
        return jnp.where(desc, rows - i, i)

    small = pltpu.make_async_copy(levels_in, levels, in_sem.at[1])
    small.start()
    loaded = pltpu.make_async_copy(u_in, raw.at[pl.ds(WIDE, rows)], in_sem.at[0])
    loaded.start()
    owners = pltpu.make_async_copy(owner_in, owner, in_sem.at[2])
    owners.start()
    barrier = pltpu.get_barrier_semaphore()
    for off in range(1, S):
        pl.semaphore_signal(barrier, inc=1, device_id={"slab": lax.rem(s + off, S)}, device_id_type=MESH)

    @pl.when(z > 0)
    def _():
        pl.semaphore_signal(barrier, inc=1, device_id={"grid": down_z}, device_id_type=MESH)

    @pl.when(z < Z - 1)
    def _():
        pl.semaphore_signal(barrier, inc=1, device_id={"grid": up_z}, device_id_type=MESH)

    pl.semaphore_wait(barrier, S - 1 + jnp.where(z > 0, 1, 0) + jnp.where(z < Z - 1, 1, 0))

    inner_halo = remote(u_in.at[pl.ds(jnp.where(descending, rows - EDGE, 0), EDGE)],
                        raw.at[pl.ds(jnp.where(descending, WIDE - EDGE, WIDE + rows), EDGE)],
                        h_send.at[0], h_recv.at[0], slab=partner)
    outer_halo = remote(u_in.at[pl.ds(jnp.where(descending, 0, rows - WIDE), WIDE)],
                        raw.at[pl.ds(jnp.where(descending, WIDE + rows, 0), WIDE)],
                        h_send.at[1], h_recv.at[1], slab=neighbour)
    inner_halo.start()
    outer_halo.start()
    small.wait()
    vec = [levels[0, d] for d in range(5)]
    scales = [lax.shift_left(jnp.int32(1), v).astype(jnp.float32) * 0.125 for v in vec]
    size = jnp.float32(1.0 / math.sqrt(Z))
    weight = jnp.where(sum(vec[1:], vec[0]) % 2 == 0, size, -size)

    sub = lax.broadcasted_iota(jnp.int32, (8, lanes), 0)
    tile = jnp.zeros((8, lanes), jnp.float32)
    for d, value in enumerate(scales + [weight]):
        tile = jnp.where(sub == d, value, tile)
    for g in range(Z):
        lv[g] = tile
    coef = coefficients(scales, descending)
    keep_mid, keep_fine = [jnp.where(3 - t <= vec[0], jnp.float32(1.0), jnp.float32(0.0)) for t in (1, 0)]
    first_w = jnp.where(descending, 0.0 * weight, weight)
    last_w = jnp.where(descending, weight, 0.0 * weight)

    send_levels = remote(lv, lv_in, h_send.at[2], h_recv.at[2], grid=main_z)
    share_levels = remote(lv, lv_in, h_send.at[3], h_recv.at[3], slab=partner)

    @pl.when(hop == 0)
    def _():
        send_levels.start()

    loaded.wait()

    inner_halo.wait_recv()

    def raw_row(i):
        r = WIDE + row_of(descending, i)
        return [raw[r, spot] for spot in spots()]

    warm_up(carry, [raw_row(i) for i in range(-STEPS, STEPS + 1)], coef)

    def first_cycle(j):
        m = march(carry, [raw_row(4 * j + 5 + i) for i in range(4)], coef)
        four = surpluses(m, first_w, last_w, weight * keep_mid, weight * keep_fine)
        order = [0, jnp.where(descending, 3, 1), 2, jnp.where(descending, 1, 3)]

        @pl.when(j < groups)
        def _():
            for k, row in zip(order, four):
                put(terms, row, 4 * group_of(descending, j) + k)

        @pl.when(j == groups)
        def _():
            for k, row in zip(order, four):
                put(o_terms, row, k + jnp.where(descending, 1, 0))
            put(o_terms, [weight * x for x in m[4]], jnp.where(descending, 0, 4))

    def piece(i, h):
        return pl.ds(4 * group_of(descending, i) + PIECE * h, PIECE)

    def main_copy(i, h):
        return remote(terms.at[piece(i, h)], arrived.at[piece(i, h)], ssem.at[i, h], rsem.at[i, h], grid=main_z)

    def halo_copy(k):
        return remote(h_terms.at[k], h_arrived.at[k], e_send.at[0, k], e_recv.at[0, k], grid=main_z)

    def outer_copy(k):
        return remote(o_terms.at[k], o_arrived.at[k], e_send.at[1, k], e_recv.at[1, k], grid=main_z)

    halo_swap = remote(h_out, h_terms, h_send.at[8], h_recv.at[8], slab=partner)

    def share_copy(i):
        where = pl.ds(OFF + 4 * group_of(region_desc, i), 4)
        return remote(sums.at[where], sums.at[where], c_send.at[i], c_recv.at[i], slab=partner)

    inner_at = OFF + jnp.where(region_desc, rows, -EDGE)
    outer_at = OFF + jnp.where(region_desc, -EDGE, rows)
    inner = pl.ds(inner_at, EDGE)
    outer = pl.ds(outer_at, EDGE)
    share_inner = remote(sums.at[inner], sums.at[inner], h_send.at[5], h_recv.at[5], slab=partner)
    share_outer = remote(sums.at[outer], sums.at[outer], h_send.at[7], h_recv.at[7], slab=partner)

    def cell(q, keeps):
        mid_keep, fine_keep = keeps
        c = [get(sums, OFF + row_of(region_desc, 4 * q + i)) for i in range(5)]
        mid = [0.5 * (a + b) + mid_keep * x for a, b, x in zip(c[0], c[4], c[2])]
        one = [0.5 * (a + b) + fine_keep * x for a, b, x in zip(c[0], mid, c[1])]
        three = [0.5 * (a + b) + fine_keep * x for a, b, x in zip(mid, c[4], c[3])]
        return [c[0], one, mid, three, c[4]]

    NC = 13

    def build_table():
        for n in range(local_grids):
            g = n + jnp.where(is_main, 0, local_grids)
            both = jnp.where(is_main, 1.0, 0.0) * lv[g] + jnp.where(is_main, 0.0, 1.0) * lv_in[g]
            lines = [jnp.broadcast_to(both[d:d + 1], (8, lanes)) for d in range(6)]
            values = coefficients(lines[:5], region_desc)
            w = lines[5]
            mid = jnp.where(lines[0] >= 0.5, 1.0, 0.0)
            fine = jnp.where(lines[0] >= 1.0, 1.0, 0.0)
            flag = jnp.where(region_desc, 1.0, 0.0)
            values = values + [mid, fine, (1.0 - flag) * w, flag * w, mid * w, fine * w]
            for k, v in enumerate(values):
                table[n, k] = v

    def table_of(n):
        values = [table[n, k] for k in range(NC + 6)]
        return values[:NC], values[NC:NC + 2], values[NC + 2:]

    def second_warm():
        for n in range(local_grids):
            c, keeps, _ = table_of(n)
            before, after = cell(-1, keeps), cell(0, keeps)
            warm_up(carry2.at[n], before[:4] + after, c)

    def second_cycle(i):
        total = None
        for n in range(local_grids):
            c, keeps, weights = table_of(n)
            m = march(carry2.at[n], cell(i + 1, keeps)[1:], c)
            rows4 = surpluses(m, *weights)
            total = rows4 if total is None else [[a + b for a, b in zip(x, y)] for x, y in zip(total, rows4)]
        r = 4 * group_of(region_desc, i)
        places = [r, r + jnp.where(region_desc, 3, 1), r + 2, r + jnp.where(region_desc, 1, 3)]
        for place, row in zip(places, total):
            for spot, value in zip(spots(), row):
                part[place, spot] = value

    def quarter(x, c):
        return pl.ds(pl.multiple_of((2 * x + c) * width, 8), width)

    def swap_copy(i, x):
        where = pl.ds(4 * group_of(region_desc, i), 4)
        return remote(part.at[where, quarter(x, 1 - core)], swapped.at[where, x], p_send.at[i, x], p_recv.at[i, x],
                      slab=partner)

    def plane_copy(i, x):
        r = 4 * group_of(region_desc, i)
        return remote(fin.at[pl.ds(r, 4), x], whole.at[pl.ds(region * rows + r, 4)],
                      x_send.at[i, x], x_recv.at[i, chip], slab=2 * x + core)

    def direct_copy(i, x, to, own, recv):
        r = 4 * group_of(region_desc, i)
        here = whole.at[pl.ds(region * rows + r, 4)]
        return remote(here if own else fin.at[pl.ds(r, 4), x], here, all_send.at[i, x, to], recv.at[i, chip],
                      grid=to, slab=2 * x + core)

    def slab_from(x, base):
        return 2 * x + (x % 2 if base == 0 else 1 - x % 2)

    def lot(i, x, base):
        m = slab_from(x, base)
        g = groups - 1 - i if m % 2 == 0 else i
        return pl.ds(m * rows + 4 * g, 4)

    def plane_arrival(i, x, base):
        return remote(fin.at[pl.ds(0, 4), 0], whole.at[lot(i, x, base)], x_send.at[i, x], x_recv.at[i, x],
                      slab=2 * x + core)

    def up_copy(i, x):
        return remote(whole.at[lot(i, x, 0)], whole.at[lot(i, x, 0)], up_send.at[i, x], up_recv.at[i, x], grid=up_z)

    def down_copy(i, x):
        return remote(whole.at[lot(i, x, 1)], whole.at[lot(i, x, 1)], dn_send.at[i, x], dn_recv.at[i, x],
                      grid=down_z)

    reach = (Z - 1) * RS_LAG
    start2 = reach + C2_LAG + 2
    swap_at = start2 + SWAP_LAG
    plane_at = swap_at + PLANE_LAG
    last = max(plane_at + groups, plane_at + (Z - 2) * CHAIN_LAG + direct_from)

    @pl.loop(0, last)
    def _(j):
        @pl.when(j == groups - 2)
        def _():
            outer_halo.wait_recv()

        @pl.when((hop == 0) & (j == 2))
        def _():
            halo_swap.wait_recv()
            for k in range(EDGE):
                halo_copy(k).start()

        @pl.when(j <= groups)
        def _():
            first_cycle(j)

            @pl.when((hop == 0) & (j < groups))
            def _():
                for h in range(4 // PIECE):
                    main_copy(j, h).start()

        @pl.when((hop == 0) & (j == groups))
        def _():
            for k in range(EDGE):
                outer_copy(k).start()

        @pl.when(j == 1)
        def _():
            e = jnp.where(descending, rows - EDGE, 0)
            for k in range(EDGE):
                put(h_out, get(terms, e + k), k)
            halo_swap.start()

        @pl.when((hop > 0) & (j == hop * RS_LAG))
        def _():
            send_levels.wait_recv()
            for g in range(Z):
                lv[g] = lv_in[g]
            lv[z] = tile

            @pl.when(hop < Z - 1)
            def _():
                send_levels.start()

            @pl.when(hop == Z - 1)
            def _():
                share_levels.start()

        b = j - hop * RS_LAG

        @pl.when((hop > 0) & (b == 2))
        def _():
            halo_swap.wait_recv()
            @pl.when(hop < Z - 1)
            def _():
                for k in range(EDGE):
                    halo_copy(k).wait_recv()
                    put(h_terms, [a + b for a, b in zip(get(h_terms, k), get(h_arrived, k))], k)
                    halo_copy(k).start()

            @pl.when(hop == Z - 1)
            def _():
                for k in range(EDGE):
                    halo_copy(k).wait_recv()
                    put(sums, [a + b for a, b in zip(get(h_terms, k), get(h_arrived, k))], inner_at + k)
                share_inner.start()

        @pl.when((hop > 0) & (b >= 0) & (b < groups))
        def _():
            @pl.when(hop < Z - 1)
            def _():
                for h in range(4 // PIECE):
                    r = 4 * group_of(descending, b) + h * PIECE
                    main_copy(b, h).wait_recv()
                    for k in range(PIECE):
                        put(terms, [a + c for a, c in zip(get(terms, r + k), get(arrived, r + k))], r + k)
                    main_copy(b, h).start()

            @pl.when(hop == Z - 1)
            def _():
                for h in range(4 // PIECE):
                    r = 4 * group_of(descending, b) + h * PIECE
                    main_copy(b, h).wait_recv()
                    for k in range(PIECE):
                        put(sums, [a + c for a, c in zip(get(terms, r + k), get(arrived, r + k))], OFF + r + k)
                share_copy(b).start()

        @pl.when((hop > 0) & (b == groups))
        def _():
            @pl.when(hop < Z - 1)
            def _():
                for k in range(EDGE):
                    outer_copy(k).wait_recv()
                    put(o_terms, [a + c for a, c in zip(get(o_terms, k), get(o_arrived, k))], k)
                    outer_copy(k).start()

            @pl.when(hop == Z - 1)
            def _():
                for k in range(EDGE):
                    outer_copy(k).wait_recv()
                    put(sums, [a + c for a, c in zip(get(o_terms, k), get(o_arrived, k))], outer_at + k)
                share_outer.start()

        i = j - start2

        @pl.when(at_end & (i == 0))
        def _():
            @pl.when(jnp.logical_not(is_main))
            def _():
                share_levels.wait_recv()
                share_inner.wait_recv()
                for k in range(min(2, groups)):
                    share_copy(k).wait_recv()
            build_table()
            second_warm()

        @pl.when(at_end & jnp.logical_not(is_main) & (i == groups - 2))
        def _():
            share_outer.wait_recv()

        @pl.when(at_end & (i >= 0) & (i < groups))
        def _():
            @pl.when(jnp.logical_not(is_main) & (i + 2 < groups))
            def _():
                share_copy(jnp.minimum(i + 2, groups - 1)).wait_recv()
            second_cycle(i)
            for x in range(chips):
                swap_copy(i, x).start()

        k = j - swap_at

        @pl.when(at_end & (k >= 0) & (k < groups))
        def _():
            r = 4 * group_of(region_desc, k)
            for x in range(chips):
                swap_copy(k, x).wait_recv()

                @pl.when(chip == x)
                def _():
                    for n in range(4):
                        whole[region * rows + r + n] = part[r + n, quarter(x, core)] + swapped[r + n, x]

                @pl.when(chip != x)
                def _():
                    for n in range(4):
                        fin[r + n, x] = part[r + n, quarter(x, core)] + swapped[r + n, x]
                    plane_copy(k, x).start()

        k2 = j - plane_at

        @pl.when((z == 0) & (k2 >= 0) & (k2 < direct_from))
        def _():
            for x in range(chips):
                @pl.when(chip != x)
                def _():
                    plane_arrival(k2, x, 0).wait_recv()
                up_copy(k2, x).start()

        @pl.when((z == Z - 1) & (k2 >= 0) & (k2 < direct_from))
        def _():
            for x in range(chips):
                @pl.when(chip != x)
                def _():
                    plane_arrival(k2, x, 1).wait_recv()
                down_copy(k2, x).start()

        @pl.when(at_end & (k2 >= direct_from) & (k2 < groups))
        def _():
            @pl.loop(1, Z)
            def _(away):
                for x in range(chips):
                    to = jnp.where(z == 0, Z - away, away - 1)

                    @pl.when((z == 0) & (chip == x))
                    def _():
                        direct_copy(k2, x, to, True, up_recv).start()

                    @pl.when((z == 0) & (chip != x))
                    def _():
                        direct_copy(k2, x, to, False, up_recv).start()

                    @pl.when((z > 0) & (chip == x))
                    def _():
                        direct_copy(k2, x, to, True, dn_recv).start()

                    @pl.when((z > 0) & (chip != x))
                    def _():
                        direct_copy(k2, x, to, False, dn_recv).start()

        f = k2 - z * CHAIN_LAG

        @pl.when((z > 0) & (z < Z - 1) & (f >= 0) & (f < direct_from))
        def _():
            for x in range(chips):
                up_copy(f, x).wait_recv()
                up_copy(f, x).start()

        d = k2 - (Z - 1 - z) * CHAIN_LAG

        @pl.when((z < Z - 1) & (z > 0) & (d >= 0) & (d < direct_from))
        def _():
            for x in range(chips):
                down_copy(d, x).wait_recv()
                down_copy(d, x).start()

    @pl.loop(0, groups)
    def _(i):
        @pl.when(hop < Z - 1)
        def _():
            for h in range(4 // PIECE):
                main_copy(i, h).wait_send()

        @pl.when(at_end & is_main)
        def _():
            share_copy(i).wait_send()

        for x in range(chips):
            @pl.when(at_end)
            def _():
                swap_copy(i, x).wait_send()

            @pl.when(at_end & (chip != x))
            def _():
                plane_copy(i, x).wait_send()

            @pl.when((z < Z - 1) & (i < direct_from))
            def _():
                up_copy(i, x).wait_send()

            @pl.when((z > 0) & (i < direct_from))
            def _():
                down_copy(i, x).wait_send()

            @pl.when(at_end & (i >= direct_from))
            def _():
                @pl.loop(1, Z)
                def _(away):
                    to = jnp.where(z == 0, Z - away, away - 1)
                    direct_copy(i, x, to, False, up_recv).wait_send()

    inner_halo.wait_send()
    outer_halo.wait_send()
    halo_swap.wait_send()

    @pl.when(hop < Z - 1)
    def _():
        for k in range(EDGE):
            halo_copy(k).wait_send()
            outer_copy(k).wait_send()
        send_levels.wait_send()

    @pl.when(at_end & is_main)
    def _():
        share_levels.wait_send()
        share_inner.wait_send()
        share_outer.wait_send()

    owners.wait()

    @pl.loop(0, groups)
    def _(i):
        for x in range(chips):
            @pl.when((z == Z - 1) | ((z > 0) & (i >= direct_from)))
            def _():
                up_copy(i, x).wait_recv()

            @pl.when((z == 0) | ((z < Z - 1) & (i >= direct_from)))
            def _():
                down_copy(i, x).wait_recv()

            @pl.when((z == 0) & (chip != x) & (i >= direct_from))
            def _():
                plane_arrival(i, x, 0).wait_recv()

            @pl.when((z == Z - 1) & (chip != x) & (i >= direct_from))
            def _():
                plane_arrival(i, x, 1).wait_recv()

    def nodal(i):
        return coarse[i // 4]

    for i in range(0, count, 4):
        coarse[i // 4] = whole[i]
    for spacing in [1 << t for t in range(2, count.bit_length() - 1)]:
        for i in range(spacing, count, 2 * spacing):
            coarse[i // 4] = nodal(i) - 0.5 * (nodal(i - spacing) + nodal((i + spacing) % count))

    for r in range(owned):
        position = owner[z * owned + r]
        top = jnp.where(position % 4 == 0, jnp.float32(1.0), jnp.float32(0.0))
        out[r] = top * coarse[position // 4] + (1.0 - top) * whole[position]


def local(field, levels, owner):
    _, rows, flat, lanes = field.shape
    Z, S = lax.axis_size("grid"), lax.axis_size("slab")
    count = owner.shape[0]
    width = flat // S
    owned = count // Z
    groups = rows // 4
    chips = S // 2
    grids = Z // 2
    tail = (TILES, N2, lanes)
    vmem = lambda *shape: pltpu.VMEM(shape, jnp.float32)
    sems = lambda *shape: pltpu.SemaphoreType.DMA(shape)
    level_tiles = vmem(Z, 8, lanes)
    hbm = pl.BlockSpec(memory_space=pltpu.HBM)
    return pl.pallas_call(
        functools.partial(kernel, (Z, S, rows, count, lanes)),
        out_shape=jax.ShapeDtypeStruct((owned, width, lanes), jnp.float32),
        in_specs=[hbm, hbm, hbm],
        out_specs=pl.BlockSpec(memory_space=pltpu.VMEM),
        scratch_shapes=[
            pltpu.SMEM(levels.shape, jnp.int32), pltpu.SMEM(owner.shape, jnp.int32),
            vmem(rows + 2 * WIDE, flat, lanes), vmem(STEPS + 1, 2, *tail), vmem(rows, *tail), vmem(rows, *tail),
            vmem(EDGE, *tail), vmem(EDGE, *tail), vmem(EDGE, *tail),
            vmem(EDGE, *tail), vmem(EDGE, *tail), vmem(OFF + rows + EDGE, *tail),
            vmem(grids, STEPS + 1, 2, *tail), vmem(rows, flat, lanes), vmem(rows, chips, width, lanes),
            vmem(rows, chips, width, lanes), vmem(count, width, lanes), vmem(count // 4, width, lanes),
            vmem(grids, 19, 8, lanes), level_tiles, level_tiles,
            sems(groups, 4 // PIECE), sems(groups, 4 // PIECE), sems(groups), sems(groups),
            sems(groups, chips), sems(groups, chips), sems(groups, chips), sems(groups, chips),
            sems(groups, chips), sems(groups, chips), sems(groups, chips), sems(groups, chips),
            sems(groups, chips, Z), sems(2, EDGE), sems(2, EDGE), sems(10), sems(10), sems(3),
        ],
        compiler_params=pltpu.CompilerParams(collective_id=0, has_side_effects=True,
                                             vmem_limit_bytes=40 * 1024 * 1024),
    )(levels, owner, field[0])


def solution(mesh):
    in_specs = (P(("copies", "grid"), "slab", None, None), P(("copies", "grid"), None), P("copies"))
    out_specs = P(("copies", "grid"), "slab", None)
    return jax.shard_map(local, mesh=mesh, in_specs=in_specs, out_specs=out_specs, check_vma=False)
```
